128 devices in a mesh: rep: 2 (over core), dp: 64 (over x, y, z).
Axes of the slice: x: 4, y: 4, z: 4, core: 2. Of those that a mesh axis runs over, the one named last changes fastest.
Arguments:
- x: bfloat16 [128, 1024, 896], P(('rep', 'dp')), parts along dimension 0
- dy: bfloat16 [128, 1024, 896], P(('rep', 'dp')), parts along dimension 0
- wq: bfloat16 [1, 896, 896], replicated
- wk: bfloat16 [1, 896, 128], replicated
- wv: bfloat16 [1, 896, 128], replicated
- wo: bfloat16 [1, 896, 896], replicated
- w_gate: bfloat16 [1, 896, 2560], replicated
- w_up: bfloat16 [1, 896, 2560], replicated
- w_down: bfloat16 [1, 2560, 896], replicated
- m_wq: float32 [1, 896, 896], replicated
- m_wk: float32 [1, 896, 128], replicated
- m_wv: float32 [1, 896, 128], replicated
- m_wo: float32 [1, 896, 896], replicated
- m_w_gate: float32 [1, 896, 2560], replicated
- m_w_up: float32 [1, 896, 2560], replicated
- m_w_down: float32 [1, 2560, 896], replicated
- v_wq: float32 [1, 896, 896], replicated
- v_wk: float32 [1, 896, 128], replicated
- v_wv: float32 [1, 896, 128], replicated
- v_wo: float32 [1, 896, 896], replicated
- v_w_gate: float32 [1, 896, 2560], replicated
- v_w_up: float32 [1, 896, 2560], replicated
- v_w_down: float32 [1, 2560, 896], replicated
Outputs:
- output 1: bfloat16 [2, 896, 896], P('rep'), parts along dimension 0
- output 2: bfloat16 [2, 896, 128], P('rep'), parts along dimension 0
- output 3: bfloat16 [2, 896, 128], P('rep'), parts along dimension 0
- output 4: bfloat16 [2, 896, 896], P('rep'), parts along dimension 0
- output 5: bfloat16 [2, 896, 2560], P('rep'), parts along dimension 0
- output 6: bfloat16 [2, 896, 2560], P('rep'), parts along dimension 0
- output 7: bfloat16 [2, 2560, 896], P('rep'), parts along dimension 0
- output 8: float32 [2, 896, 896], P('rep'), parts along dimension 0
- output 9: float32 [2, 896, 128], P('rep'), parts along dimension 0
- output 10: float32 [2, 896, 128], P('rep'), parts along dimension 0
- output 11: float32 [2, 896, 896], P('rep'), parts along dimension 0
- output 12: float32 [2, 896, 2560], P('rep'), parts along dimension 0
- output 13: float32 [2, 896, 2560], P('rep'), parts along dimension 0
- output 14: float32 [2, 2560, 896], P('rep'), parts along dimension 0
- output 15: float32 [2, 896, 896], P('rep'), parts along dimension 0
- output 16: float32 [2, 896, 128], P('rep'), parts along dimension 0
- output 17: float32 [2, 896, 128], P('rep'), parts along dimension 0
- output 18: float32 [2, 896, 896], P('rep'), parts along dimension 0
- output 19: float32 [2, 896, 2560], P('rep'), parts along dimension 0
- output 20: float32 [2, 896, 2560], P('rep'), parts along dimension 0
- output 21: float32 [2, 2560, 896], P('rep'), parts along dimension 0
There are 2 independent parts. The reference program is written for one: setup_inputs(seed, part) draws one part's arguments, and reference() takes and returns one part's arrays. A program takes and returns all parts, laid end to end along the dimension named above; an argument that names none is the same for every part.
All inputs are finite; a program needn't handle non-finite values.
Results may differ from the reference program's by a relative error of at most 0.024.
Values are sent between devices in bfloat16 or wider.
A program may use at most 1.5 GiB of HBM per device.

```python
import jax
import jax.numpy as jnp
from jax import lax

SEQUENCES = 64
TOKENS = 1024
D = 896
HEADS = 7
KV_HEADS = 1
HEAD = 128
FF = 2560
LAYERS = 1
THETA = 10000
NAMES = ("wq", "wk", "wv", "wo", "w_gate", "w_up", "w_down")
SHAPES = {
    "wq": (LAYERS, D, HEADS * HEAD),
    "wk": (LAYERS, D, KV_HEADS * HEAD),
    "wv": (LAYERS, D, KV_HEADS * HEAD),
    "wo": (LAYERS, HEADS * HEAD, D),
    "w_gate": (LAYERS, D, FF),
    "w_up": (LAYERS, D, FF),
    "w_down": (LAYERS, FF, D),
}


def bump(key, n, height):
    away = (jnp.arange(n, dtype=jnp.int32) - jax.random.randint(key, (), 0, n, jnp.int32)) % n
    return jnp.where(away < n // 8, height, 1.0)


def together(key, own, strength):
    shared = jax.random.normal(key, own.shape[1:], jnp.float32)
    return (own + strength * shared) * lax.rsqrt(1 + strength * strength)


def setup_inputs(seed: int = 0, part: int = 0) -> dict:
    kx, kdy, ka, kb, kz, kf, kh, kl, *keys = jax.random.split(jax.random.key(seed), 8 + 3 * len(NAMES))
    kx, kdy, ka, kb = (jax.random.fold_in(k, part) for k in (kx, kdy, ka, kb))
    kw, km, kv = (keys[i::3] for i in range(3))
    shape = (SEQUENCES, TOKENS, D)
    much_x, much_dy = jax.random.uniform(kz, (2,), jnp.float32, 0.0, 1.0)
    loud = 2.0 ** jax.random.uniform(jax.random.fold_in(kz, 1), (), jnp.float32, -1.0, 2.0)
    layers = 2.0 ** jax.random.uniform(kl, (LAYERS, 1, 1), jnp.float32, -1.0, 1.0)
    times = {"wq": 1.0, "wk": 1.0, "wv": 2.0, "wo": layers, "w_gate": 1.0, "w_up": bump(kh, FF, 4.0), "w_down": layers}
    x = together(ka, jax.random.normal(kx, shape, jnp.float32), much_x) * bump(kf, D, 4.0)
    dy = together(kb, jax.random.normal(kdy, shape, jnp.float32), much_dy)
    drawn = {"x": x.astype(jnp.bfloat16), "dy": (loud * dy * (SEQUENCES * TOKENS) ** -0.5).astype(jnp.bfloat16)}
    for key, name in zip(kw, NAMES, strict=True):
        drawn[name] = (jax.random.normal(key, SHAPES[name], jnp.float32) * SHAPES[name][1] ** -0.5 * times[name]).astype(jnp.bfloat16)
    for key, name in zip(km, NAMES, strict=True):
        drawn[f"m_{name}"] = 0.1 * jax.random.normal(key, SHAPES[name], jnp.float32)
    for key, name in zip(kv, NAMES, strict=True):
        drawn[f"v_{name}"] = loud * loud * jax.random.uniform(key, SHAPES[name], jnp.float32, 0.2, 0.6)
    return drawn


def matmul(a, w):
    return jnp.dot(a, w, preferred_element_type=jnp.float32).astype(jnp.bfloat16)


def normed(h):
    wide = h.astype(jnp.float32)
    scale = lax.rsqrt(jnp.mean(wide**2, -1, keepdims=True) + 1e-6)
    return (wide * scale).astype(jnp.bfloat16)


def turned(t, theta):
    half = t.shape[-1] // 2
    angle = jnp.arange(t.shape[0], dtype=jnp.float32)[:, None] * theta ** (-jnp.arange(half, dtype=jnp.float32) / half)
    cos, sin = jnp.cos(angle)[:, None], jnp.sin(angle)[:, None]
    a, b = t[..., :half].astype(jnp.float32), t[..., half:].astype(jnp.float32)
    return jnp.concatenate([a * cos - b * sin, b * cos + a * sin], -1).astype(jnp.bfloat16)


def seen_by(q, k, v):
    tokens, kv = q.shape[0], k.shape[1]
    q = q.reshape(tokens, kv, -1, q.shape[-1])
    scores = jnp.einsum("tgsd,ugd->gstu", q.astype(jnp.float32), k.astype(jnp.float32)) * q.shape[-1] ** -0.5
    place = jnp.arange(tokens)
    weights = jax.nn.softmax(jnp.where(place[:, None] >= place, scores, -jnp.inf), -1).astype(jnp.bfloat16)
    return jnp.einsum("gstu,ugd->tgsd", weights.astype(jnp.float32), v.astype(jnp.float32)).astype(jnp.bfloat16).reshape(tokens, -1)


def layer(h, w):
    a = normed(h)
    q, k = (turned(matmul(a, w[name]).reshape(h.shape[0], -1, HEAD), THETA) for name in ("wq", "wk"))
    h = h + matmul(seen_by(q, k, matmul(a, w["wv"]).reshape(h.shape[0], -1, HEAD)), w["wo"])
    b = normed(h)
    gate = jnp.dot(b, w["w_gate"], preferred_element_type=jnp.float32)
    up = jnp.dot(b, w["w_up"], preferred_element_type=jnp.float32)
    return h + matmul((jax.nn.silu(gate) * up).astype(jnp.bfloat16), w["w_down"])


def adamw(w, m, v, g):
    m = 0.9 * m + 0.1 * g
    v = 0.95 * v + 0.05 * g * g
    step = m * lax.rsqrt(v + 1e-8) + 0.1 * w
    return (w - 0.02 * step).astype(jnp.bfloat16), m, v


def stack(weights, h):
    return lax.scan(lambda h, w: (layer(h, w), None), h, weights)[0]


def reference(x, dy, wq, wk, wv, wo, w_gate, w_up, w_down, m_wq, m_wk, m_wv, m_wo, m_w_gate, m_w_up, m_w_down, v_wq, v_wk, v_wv, v_wo, v_w_gate, v_w_up, v_w_down):
    weights = dict(zip(NAMES, (wq, wk, wv, wo, w_gate, w_up, w_down), strict=True))

    def take(so_far, sequence):
        h, by_y = sequence
        _, back = jax.vjp(stack, weights, h)
        by_weights, by_h = back(by_y)
        return jax.tree.map(lambda total, term: total + term.astype(jnp.float32), so_far, by_weights), by_h

    none_yet = {name: jnp.zeros(w.shape, jnp.float32) for name, w in weights.items()}
    by_weights, by_x = lax.scan(take, none_yet, (x, dy))
    gradients = [by_weights[name].astype(jnp.bfloat16).astype(jnp.float32) for name in NAMES]
    first = (m_wq, m_wk, m_wv, m_wo, m_w_gate, m_w_up, m_w_down)
    second = (v_wq, v_wk, v_wv, v_wo, v_w_gate, v_w_up, v_w_down)
    new = [adamw(weights[name].astype(jnp.float32), m, v, g) for name, m, v, g in zip(NAMES, first, second, gradients, strict=True)]
    return tuple(one[which] for which in range(3) for one in new)
```

```python
import functools

import jax
import jax.numpy as jnp
import numpy as np
from jax import lax
from jax.experimental import pallas as pl
from jax.experimental.pallas import tpu as pltpu
from jax.sharding import PartitionSpec as P

HEAD = 128
HALF = HEAD // 2
HEADS = 7
THETA = 10000
TOKENS = 1024
D, FF, QKV = 896, 2560, 1152
QB = 256
PART = FF // 4
SCALE = HEAD**-0.5
LOG2E = 1.4426950408889634
LAST = 11
STRIDES = (16, 4, 1)
MESH_ID = pl.DeviceIdType.MESH
SLABS = ((0, 256), (256, 320), (576, 320))
CUTS = ((0, 256), (256, 192), (448, 192))
bf16, f32 = jnp.bfloat16, jnp.float32


def dot(a, b, ca=1, cb=0):
    return lax.dot_general(a, b, (((ca,), (cb,)), ((), ())), preferred_element_type=f32)


def dot_t(a, b):
    return dot(a, b, 1, 1)


def scale_of(h):
    return lax.rsqrt(jnp.mean(h * h, 0, keepdims=True) + 1e-6)


def normed(h):
    wide = h.astype(f32)
    return (wide * scale_of(wide)).astype(bf16)


def adamw(w, m, v, g):
    m = 0.9 * m + 0.1 * g
    v = 0.95 * v + 0.05 * g * g
    step = m * lax.rsqrt(v + 1e-8) + 0.1 * w
    return (w - 0.02 * step).astype(bf16), m, v


def hidden():
    return lax.broadcasted_iota(jnp.int32, (QB, QB), 0) > lax.broadcasted_iota(jnp.int32, (QB, QB), 1)


def turn(t, cos, sin):
    a, b = t[:HALF].astype(f32), t[HALF:].astype(f32)
    return jnp.concatenate([a * cos - b * sin, b * cos + a * sin], 0).astype(bf16)


def attend_kernel(q_in, k_in, v_ref, cos_ref, sin_ref, out_ref, lse_ref, q_ref, kt_ref, k_ref, v_out):
    @pl.when(pl.program_id(0) == 0)
    def _():
        kt_ref[...] = turn(k_in[...], cos_ref[...], sin_ref[...])
        k_ref[...] = kt_ref[...].T
        v_out[...] = v_ref[...].T

    q_ref[...] = turn(q_in[...], cos_ref[...], sin_ref[...])
    for i in range(TOKENS // QB):
        cols, seen = slice(i * QB, (i + 1) * QB), i * QB
        q = q_ref[:, cols]
        edge = jnp.where(hidden(), -1e30, dot(k_ref[cols, :], q))
        top = edge.max(0, keepdims=True)
        if seen:
            past = dot(k_ref[:seen, :], q)
            top = jnp.maximum(top, past.max(0, keepdims=True))
        p = jnp.exp2((edge - top) * (SCALE * LOG2E))
        total, got = p.sum(0, keepdims=True), dot(v_ref[:, cols], p.astype(bf16))
        if seen:
            p = jnp.exp2((past - top) * (SCALE * LOG2E))
            total, got = total + p.sum(0, keepdims=True), got + dot(v_ref[:, :seen], p.astype(bf16))
        out_ref[:, cols] = (got * (1 / total)).astype(bf16)
        lse_ref[0, :, cols] = top * SCALE + jnp.log(total)


def attend(qkv, cos, sin):
    table, tall = pl.BlockSpec((HALF, TOKENS), lambda i: (0, 0)), pl.BlockSpec((TOKENS, HEAD), lambda i: (0, 0))
    row = lambda at: pl.BlockSpec((HEAD, TOKENS), at)
    each = row(lambda i: (i, 0))
    like = jax.ShapeDtypeStruct
    return pl.pallas_call(
        attend_kernel,
        grid=(HEADS,),
        in_specs=[each, row(lambda i: (HEADS, 0)), row(lambda i: (HEADS + 1, 0)), table, table],
        out_specs=[each, pl.BlockSpec((1, 1, TOKENS), lambda i: (i, 0, 0)), each, row(lambda i: (0, 0)), tall, tall],
        out_shape=[like((D, TOKENS), bf16), like((HEADS, 1, TOKENS), f32), like((D, TOKENS), bf16), like((HEAD, TOKENS), bf16),
                   like((TOKENS, HEAD), bf16), like((TOKENS, HEAD), bf16)],
        compiler_params=pltpu.CompilerParams(vmem_limit_bytes=32 * 2**20),
        name="attend",
    )(qkv, qkv, qkv, cos, sin)


def hidden_kernel(wg_ref, wu_ref, wd_ref, b_ref, dy_ref, act_ref, dg_ref, du_ref):
    gate, up = dot(wg_ref[...], b_ref[...], 0, 0), dot(wu_ref[...], b_ref[...], 0, 0)
    back = dot(wd_ref[...], dy_ref[...]).astype(bf16).astype(f32)
    sig = 1 / (1 + jnp.exp(-gate))
    silu = gate * sig
    act_ref[...] = (silu * up).astype(bf16)
    du_ref[...] = (back * silu).astype(bf16)
    dg_ref[...] = (back * up * (sig + silu * (1 - sig))).astype(bf16)


def hidden_units(wg, wu, wd, b, dy):
    wide, whole = pl.BlockSpec((D, QB), lambda i: (0, i)), pl.BlockSpec((D, TOKENS), lambda i: (0, 0))
    out = pl.BlockSpec((QB, TOKENS), lambda i: (i, 0))
    return pl.pallas_call(
        hidden_kernel,
        grid=(FF // QB,),
        in_specs=[wide, wide, pl.BlockSpec((QB, D), lambda i: (i, 0)), whole, whole],
        out_specs=[out] * 3,
        out_shape=[jax.ShapeDtypeStruct((FF, TOKENS), bf16)] * 3,
        compiler_params=pltpu.CompilerParams(vmem_limit_bytes=48 * 2**20),
        name="hidden_units",
    )(wg, wu, wd, b, dy)


class Unit:
    def __init__(self, number, wave, colour, row0, rows, cols):
        self.n, self.wave, self.axes, self.row0, self.R, self.W = number, wave, tuple((colour + i) % 3 for i in range(3)), row0, rows, cols
        self.Rb = rows // 4
        self.h = -(-self.Rb // 32) * 16


def waves_of():
    got = [[Unit(c, 0, c, row0, rows, D) for c, (row0, rows) in enumerate(CUTS)]]
    for wave, cols in ((1, PART), (2, PART), (3, 512)):
        got.append([Unit(3 * wave + c, wave, c, row0, rows, cols) for c, (row0, rows) in enumerate(SLABS)])
    return got


def pieces(u):
    r = slice(u.row0, u.row0 + u.R)
    if u.wave == 0:
        return [(6, slice(j * PART + u.row0, j * PART + u.row0 + u.R), slice(0, D), j, slice(0, D)) for j in range(4)]
    if u.wave < 3:
        return [(3 + u.wave, r, slice(j * PART, (j + 1) * PART), j, slice(0, PART)) for j in range(4)]
    cut = ((0, 0, 512, 0, 0), (0, 512, D, 1, 0), (1, 0, HEAD, 1, 384), (2, 0, HEAD, 2, 0), (3, 0, 384, 2, HEAD), (3, 384, D, 3, 0))
    return [(a, r, slice(c0, c1), j, slice(b0, b0 + c1 - c0)) for a, c0, c1, j, b0 in cut]


class Comm:
    def __init__(self, units, bufs, ssem, rsem):
        self.units, self.bufs, self.ssem, self.rsem = units, bufs, ssem, rsem
        self.rep, self.me = lax.axis_index("rep"), lax.axis_index("dp")
        self.at = [lax.rem(lax.div(self.me, s), 4) for s in STRIDES]

    def place(self, u, stage):
        p = self.at[u.axes[stage]]
        return p, lax.rem(p + 1, 4), lax.rem(p + 3, 4), lax.rem(p + 2, 4)

    def neighbour(self, axis, by):
        p = self.at[axis]
        return self.me + (lax.rem(p + by, 4) - p) * STRIDES[axis]

    def barrier(self):
        sem = pltpu.get_barrier_semaphore()
        for axis in range(3):
            for by in (1, 3):
                pl.semaphore_signal(sem, inc=1, device_id=(self.rep, self.neighbour(axis, by)), device_id_type=MESH_ID)
        pl.semaphore_wait(sem, 6)

    def copy(self, u, stage, k, src, dst, by):
        return pltpu.make_async_remote_copy(src_ref=src, dst_ref=dst, send_sem=self.ssem.at[u.n, k], recv_sem=self.rsem.at[u.n, k],
                                            device_id=(self.rep, self.neighbour(u.axes[stage], by)), device_id_type=MESH_ID)

    def send(self, u, stage, k, src, dst, by):
        self.copy(u, stage, k, src, dst, by).start()

    def got(self, u, stage, k, dst):
        self.copy(u, stage, k, dst, dst, 1).wait_recv()

    def done_sending(self, u, stage, k, parts):
        for i, part in enumerate(parts):
            self.copy(u, stage, k + i, part, part, 1).wait_send()

    @staticmethod
    def rows(ref, start, n):
        return ref.at[pl.ds(start if isinstance(start, int) else pl.multiple_of(start, 16), n), :]

    @staticmethod
    def each(n, f):
        rows = next(size for size in (64, 48, 32, 16) if n % size == 0)

        def body(i, _):
            f(pl.multiple_of(i * rows, 16), rows)

        lax.fori_loop(0, n // rows, body, None)

    def scatter_start(self, u, stage):
        b = self.bufs[u.n]
        p, r, l, o = self.place(u, stage)
        if stage == 0:
            size, h, src = u.R, u.R // 2, lambda j, at, n: self.rows(b.own.at[j], at, n)
            ro, rr = b.r1o, b.r1
        else:
            size, h, src = u.Rb, u.h, lambda j, at, n: self.rows(b.r1o, j * u.Rb + at, n)
            ro, rr = b.r2o, b.r2
        k = 6 * stage
        self.send(u, stage, k, src(o, 0, h), ro.at[0:h], 1)
        self.send(u, stage, k + 1, src(o, h, size - h), ro.at[h:size], 3)
        self.send(u, stage, k + 2, src(r, h, size - h), rr.at[0, h:size], 1)
        self.send(u, stage, k + 3, src(l, 0, h), rr.at[1, 0:h], 3)

    def scatter_combine(self, u, stage):
        b = self.bufs[u.n]
        p, r, l, o = self.place(u, stage)
        size, h, ro, rr = (u.R, u.R // 2, b.r1o, b.r1) if stage == 0 else (u.Rb, u.h, b.r2o, b.r2)
        k = 6 * stage
        for step, (j, lo, n, by, slot) in enumerate(((r, 0, h, 1, 0), (l, h, size - h, 3, 1))):
            self.got(u, stage, k + step, ro.at[lo : lo + n])

            def add(i, size):
                here = pl.ds(pl.multiple_of(lo + i, 16), size)
                ro[here, :] = (self.term(u, stage, j, lo + i, size) + ro[here, :].astype(jnp.float32)).astype(jnp.bfloat16)

            self.each(n, add)
            self.send(u, stage, k + 4 + step, ro.at[lo : lo + n], rr.at[slot, lo : lo + n], by)

    def term(self, u, stage, j, at, size):
        b = self.bufs[u.n]
        if stage == 0:
            return b.own[j, pl.ds(pl.multiple_of(at, 16), size), :].astype(jnp.float32)
        here = pl.ds(pl.multiple_of(j * u.Rb + at, 16), size)
        return self.first_sum(u, here)

    def first_sum(self, u, here):
        b = self.bufs[u.n]
        mine = self.place(u, 0)[0]
        return b.own[mine, here, :].astype(jnp.float32) + b.r1[0, here, :].astype(jnp.float32) + b.r1[1, here, :].astype(jnp.float32)

    def scatter_wait(self, u, stage):
        b = self.bufs[u.n]
        size, h, rr = (u.R, u.R // 2, b.r1) if stage == 0 else (u.Rb, u.h, b.r2)
        k = 6 * stage
        self.got(u, stage, k + 2, rr.at[0, h:size])
        self.got(u, stage, k + 3, rr.at[1, 0:h])
        self.got(u, stage, k + 4, rr.at[0, 0:h])
        self.got(u, stage, k + 5, rr.at[1, h:size])
        one, other = (b.r1o, b.r2o)[stage].at[0:h], (b.r1o, b.r2o)[stage].at[h:size]
        self.done_sending(u, stage, k, (one, other, other, one, one, other))

    def first_end(self, u):
        b = self.bufs[u.n]
        self.scatter_wait(u, 0)

        def add(i, size):
            here = pl.ds(i, size)
            b.r1o[here, :] = self.first_sum(u, here).astype(jnp.bfloat16)

        self.each(u.R, add)
        self.scatter_start(u, 1)

    def second_end(self, u):
        b = self.bufs[u.n]
        self.scatter_wait(u, 1)
        mine, slot = self.place(u, 1)[0], self.place(u, 2)[0]

        def add(i, size):
            here = pl.ds(i, size)
            total = self.term(u, 1, mine, i, size) + b.r2[0, here, :].astype(jnp.float32) + b.r2[1, here, :].astype(jnp.float32)
            b.t3[slot, here, :] = total.astype(jnp.bfloat16)

        self.each(u.Rb, add)
        self.gather_start(u, 2)

    def region(self, u, stage):
        b = self.bufs[u.n]
        if stage == 2:
            return (lambda j, at, n: b.t3.at[j, at : at + n]), u.Rb, u.h, 12
        if stage == 1:
            mine = self.place(u, 0)[0]
            return (lambda j, at, n: self.rows(b.own.at[mine], j * u.Rb + at, n)), u.Rb, u.h, 16
        return (lambda j, at, n: b.own.at[j, at : at + n]), u.R, u.R // 2, 20

    def gather_start(self, u, stage):
        part, size, h, k = self.region(u, stage)
        p, r, l, o = self.place(u, stage)
        self.send(u, stage, k, part(p, 0, size), part(p, 0, size), 1)
        self.send(u, stage, k + 1, part(p, 0, size), part(p, 0, size), 3)

    def gather_forward(self, u, stage):
        part, size, h, k = self.region(u, stage)
        p, r, l, o = self.place(u, stage)
        self.got(u, stage, k, part(l, 0, size))
        self.send(u, stage, k + 2, part(l, 0, h), part(l, 0, h), 1)
        self.got(u, stage, k + 1, part(r, 0, size))
        self.send(u, stage, k + 3, part(r, h, size - h), part(r, h, size - h), 3)

    def gather_wait(self, u, stage):
        part, size, h, k = self.region(u, stage)
        p, r, l, o = self.place(u, stage)
        self.got(u, stage, k + 2, part(o, 0, h))
        self.got(u, stage, k + 3, part(o, h, size - h))
        self.done_sending(u, stage, k, (part(p, 0, size), part(p, 0, size), part(l, 0, h), part(r, h, size - h)))

    def third_end(self, u):
        b = self.bufs[u.n]
        self.gather_wait(u, 2)
        first, second = self.place(u, 0)[0], self.place(u, 1)[0]

        def add(i, size):
            here = pl.ds(i, size)
            a, c, d, e = (b.t3[j, here, :].astype(jnp.float32) for j in range(4))
            b.own[first, pl.ds(pl.multiple_of(second * u.Rb + i, 16), size), :] = (a + c + d + e).astype(jnp.bfloat16)

        self.each(u.Rb, add)
        self.gather_start(u, 1)

    def fourth_end(self, u):
        self.gather_wait(u, 1)
        self.gather_start(u, 0)

    def stage(self, wave, number):
        steps = ((self.scatter_start, 0), (self.scatter_combine, 0), (self.first_end,), (self.scatter_combine, 1), (self.second_end,),
                 (self.gather_forward, 2), (self.third_end,), (self.gather_forward, 1), (self.fourth_end,), (self.gather_forward, 0), (self.gather_wait, 0))
        for u in wave:
            steps[number][0](u, *steps[number][1:])


class Bufs:
    def __init__(self, refs):
        self.own, self.r1o, self.r1, self.r2o, self.r2, self.t3 = refs


def unit_scratch(u):
    shapes = ((4, u.R, u.W), (u.R, u.W), (2, u.R, u.W), (u.Rb, u.W), (2, u.Rb, u.W), (4, u.Rb, u.W))
    return [pltpu.VMEM(s, bf16) for s in shapes]


BESIDE = "/0/1//01/2/01/012/012/012/01/12//12/".split("/")
AFTER = "312333032303230323"


class Pacer:
    def __init__(self, comm, waves, finish):
        self.comm, self.waves, self.finish = comm, waves, finish
        self.next, self.plan = {}, list(BESIDE)

    def launch(self, w):
        self.comm.stage(self.waves[w], 0)
        self.next[w] = 1

    def advance(self, order):
        for w in map(int, order):
            self.comm.stage(self.waves[w], self.next[w])
            self.next[w] += 1
            if self.next[w] == LAST:
                self.finish(w)

    def tick(self):
        self.advance(self.plan.pop(0))


def turn_back(d, cos, sin):
    d = d.astype(bf16).astype(f32)
    a, b = d[:HALF], d[HALF:]
    return jnp.concatenate([a * cos + b * sin, b * cos - a * sin], 0).astype(bf16)


def main_kernel(act, dg, du, dy, b, h, out, a, q, kt, k, v, lse, cos, sin, wg, wu, wo, *refs):
    waves = waves_of()
    units = [u for wave in waves for u in wave]
    outs, scratch = refs[:7], refs[7:]
    bufs = [Bufs(scratch[6 * n : 6 * n + 6]) for n in range(len(units))]
    ssem, rsem, osem, dy_s, db_s, csem, wsem, isem = scratch[6 * len(units) :]
    comm = Comm(units, bufs, ssem, rsem)

    def results(u):
        for i, (n, r, c, j, cols) in enumerate(pieces(u)):
            yield pltpu.make_async_copy(bufs[u.n].own.at[j, :, cols], outs[n].at[r, c], osem.at[u.n, i])

    def finish(w):
        for u in waves[w]:
            for copy in results(u):
                copy.start()

    pacer = Pacer(comm, waves, finish)

    def keep(w, j, cols, got):
        for u in waves[w]:
            bufs[u.n].own[j, :, cols] = got[u.row0 : u.row0 + u.R].astype(bf16)

    def first(chunk, weight, b_s):
        dy_in, b_in = pltpu.make_async_copy(dy, dy_s, isem.at[0]), pltpu.make_async_copy(b, b_s, isem.at[1])
        groups = [(w, j, False) for w in range(3) for j in (0, 2)] + [(w, j, True) for w in (1, 2) for j in (0, 2)]

        def loads(g):
            w, start, back = groups[g]
            for i in range(2):
                slot, j = g % 2 * 2 + i, start + i
                yield pltpu.make_async_copy((act, dg, du)[w].at[j * PART : (j + 1) * PART, :], chunk.at[slot], csem.at[slot])
                if back:
                    yield pltpu.make_async_copy((wg, wu)[w - 1].at[:, j * PART : (j + 1) * PART], weight.at[slot], wsem.at[slot])

        def run(g):
            w, start, back = groups[g]

            def body(i, _):
                slot, j = g % 2 * 2 + i, start + i
                if w == 0:
                    keep(0, j, slice(0, D), dot_t(chunk[slot], dy_s[...]))
                elif not back:
                    keep(w, j, slice(0, PART), dot_t(b_s[...], chunk[slot]))
                else:

                    def some(n, _):
                        cols = pl.ds(pl.multiple_of(n * QB, QB), QB)
                        db_s[:, cols] += dot(weight[slot], chunk[slot, :, cols])

                    lax.fori_loop(0, TOKENS // QB, some, None)

            lax.fori_loop(0, 2, body, None)

        for copy in [dy_in, *loads(0), b_in]:
            copy.start()
        db_s[...] = jnp.zeros_like(db_s)
        dy_in.wait()
        for g, (w, start, back) in enumerate(groups):
            if g + 1 < len(groups):
                for copy in loads(g + 1):
                    copy.start()
            for copy in loads(g):
                copy.wait()
            if (w, start, back) == (1, 0, False):
                b_in.wait()
            run(g)
            if start and not back:
                if w == 0:
                    comm.barrier()
                pacer.launch(w)
            if w:
                pacer.tick()

    def second(h_s, out_s, wo_s, q_s, kt_s, k_s, v_s, lse_s, cos_s, sin_s, dout_s, dqkv_s, dk_s, dv_s, delta_s):
        near, far = (h_s, out_s, wo_s, q_s, kt_s, k_s, v_s, lse_s, cos_s, sin_s), (h, out, wo, q, kt, k, v, lse, cos, sin)
        ins = [pltpu.make_async_copy(x, y, isem.at[n]) for n, (x, y) in enumerate(zip(far, near))]
        for copy in ins:
            copy.start()
        dk_s[...] = jnp.zeros_like(dk_s)
        dv_s[...] = jnp.zeros_like(dv_s)
        for copy in ins:
            copy.wait()

        def through_norm(i, _):
            cols = pl.ds(pl.multiple_of(i * HEAD, HEAD), HEAD)
            x, g = h_s[:, cols].astype(f32), db_s[:, cols].astype(bf16).astype(f32)
            s = scale_of(x)
            d = g * s - x * (s * s * s * jnp.mean(g * x, 0, keepdims=True))
            h_s[:, cols] = (d.astype(bf16).astype(f32) + dy_s[:, cols].astype(f32)).astype(bf16)

        lax.fori_loop(0, TOKENS // HEAD, through_norm, None)
        pacer.tick()
        dout_s[...] = dot(wo_s[...], h_s[...]).astype(bf16)
        pacer.tick()
        keep(3, 2, slice(HEAD, 512), dot_t(out_s[...], h_s[:384, :]))
        keep(3, 3, slice(0, 512), dot_t(out_s[...], h_s[384:, :]))
        pacer.tick()
        for n in range(HEADS):
            rows = slice(n * HEAD, (n + 1) * HEAD)
            delta_s[n] = (dout_s[rows, :].astype(f32) * out_s[rows, :].astype(f32)).sum(0, keepdims=True)
        a_in = pltpu.make_async_copy(a, out_s, isem.at[1])
        a_in.start()

        def head(n, _):
            rows = pl.ds(pl.multiple_of(n * HEAD, HEAD), HEAD)
            for i in range(TOKENS // QB):
                cols, seen = slice(i * QB, (i + 1) * QB), i * QB
                qi, do = q_s[rows, cols], dout_s[rows, cols]
                top, delta = lse_s[n][:, cols] * LOG2E, delta_s[n][:, cols]
                dq = None
                for keys in [slice(0, seen), cols] if seen else [cols]:
                    p = jnp.exp2(dot(k_s[keys, :], qi) * (SCALE * LOG2E) - top)
                    if keys is cols:
                        p = jnp.where(hidden(), 0.0, p)
                    ds = (p * (dot(v_s[keys, :], do) - delta)).astype(bf16)
                    dv_s[:, keys] += dot_t(do, p.astype(bf16))
                    dk_s[:, keys] += dot_t(qi, ds)
                    part = dot(kt_s[:, keys], ds)
                    dq = part if dq is None else dq + part
                dqkv_s[rows, cols] = turn_back(dq * SCALE, cos_s[:, cols], sin_s[:, cols])

        for n in range(0, HEADS, 2):
            lax.fori_loop(n, min(n + 2, HEADS), head, None)
            pacer.tick()
        dqkv_s[D : D + HEAD, :] = turn_back(dk_s[...] * SCALE, cos_s[...], sin_s[...])
        dqkv_s[D + HEAD :, :] = dv_s[...].astype(bf16)
        a_in.wait()
        for j, start, n in ((0, 0, 512), (1, 512, 512), (2, D + HEAD, HEAD)):
            keep(3, j, slice(0, n), dot_t(out_s[...], dqkv_s[start : start + n, :]))
        pacer.launch(3)

    wide = pltpu.VMEM((D, TOKENS), bf16)
    pl.run_scoped(first, pltpu.VMEM((4, PART, TOKENS), bf16), pltpu.VMEM((4, D, PART), bf16), wide)
    small, tall = pltpu.VMEM((HEAD, TOKENS), bf16), pltpu.VMEM((TOKENS, HEAD), bf16)
    table, row = pltpu.VMEM((HALF, TOKENS), f32), pltpu.VMEM((HEADS, 1, TOKENS), f32)
    sums = pltpu.VMEM((HEAD, TOKENS), f32)
    pl.run_scoped(second, wide, wide, pltpu.VMEM((D, D), bf16), wide, small, tall, tall, row, table, table, wide, pltpu.VMEM((QKV, TOKENS), bf16), sums, sums, row)
    pacer.advance(AFTER)
    for u in units:
        for copy in results(u):
            copy.wait()


def gradients(*arrays):
    units = [u for wave in waves_of() for u in wave]
    anywhere = pl.BlockSpec(memory_space=pl.ANY)
    shapes = ((D, D), (D, HEAD), (D, HEAD), (D, D), (D, FF), (D, FF), (FF, D))
    dma = pltpu.SemaphoreType.DMA
    return pl.pallas_call(
        main_kernel,
        out_shape=[jax.ShapeDtypeStruct(s, bf16) for s in shapes],
        in_specs=[anywhere] * len(arrays),
        out_specs=[anywhere] * len(shapes),
        scratch_shapes=[s for u in units for s in unit_scratch(u)]
        + [dma((len(units), 24)), dma((len(units), 24)), dma((len(units), 6)), pltpu.VMEM((D, TOKENS), bf16), pltpu.VMEM((D, TOKENS), f32), dma((4,)), dma((4,)), dma((10,))],
        compiler_params=pltpu.CompilerParams(collective_id=0, has_side_effects=True, vmem_limit_bytes=63 * 2**20),
        name="gradients",
    )(*arrays)


def solution(mesh):
    def step(x, dy, *arrays):
        weights, m, v = (arrays[i : i + 7] for i in (0, 7, 14))
        wq, wk, wv, wo, wg, wu, wd = (w[0] for w in weights)
        x, dy = x[0].T, dy[0].T
        angle = jnp.arange(TOKENS, dtype=f32)[None, :] * THETA ** (-jnp.arange(HALF, dtype=f32) / HALF)[:, None]
        cos, sin = jnp.cos(angle), jnp.sin(angle)
        a = normed(x)
        qkv = dot(jnp.concatenate([wq, wk, wv], 1), a, 0, 0).astype(bf16)
        out, lse, q, kt, k, v_tall = attend(qkv, cos, sin)
        h = x + dot(wo, out, 0, 0).astype(bf16)
        b = normed(h)
        act, dg, du = hidden_units(wg, wu, wd, b, dy)
        summed = gradients(act, dg, du, dy, b, h, out, a, q, kt, k, v_tall, lse, cos, sin, wg, wu, wo)
        new = [adamw(w.astype(f32), m, v, g[None].astype(f32)) for w, m, v, g in zip(weights, m, v, summed, strict=True)]
        return tuple(one[which] for which in range(3) for one in new)

    states, all_of = P(("rep", "dp"), None, None), P(None, None, None)
    return jax.shard_map(
        step,
        mesh=mesh,
        in_specs=(states, states) + (all_of,) * 21,
        out_specs=(P("rep", None, None),) * 21,
        check_vma=False,
    )
```

```python
import functools

import jax
import jax.numpy as jnp
import numpy as np
from jax import lax
from jax.experimental import pallas as pl
from jax.experimental.pallas import tpu as pltpu
from jax.sharding import PartitionSpec as P

HEAD = 128
HALF = HEAD // 2
HEADS = 7
THETA = 10000
TOKENS = 1024
D, FF, QKV = 896, 2560, 1152
QB = 256
PART = FF // 4
SCALE = HEAD**-0.5
LOG2E = 1.4426950408889634
LAST = 11
STRIDES = (16, 4, 1)
MESH_ID = pl.DeviceIdType.MESH
SLABS = ((0, 256), (256, 320), (576, 320))
CUTS = ((0, 256), (256, 192), (448, 192))
bf16, f32 = jnp.bfloat16, jnp.float32


def dot(a, b, ca=1, cb=0):
    return lax.dot_general(a, b, (((ca,), (cb,)), ((), ())), preferred_element_type=f32)


def dot_t(a, b):
    return dot(a, b, 1, 1)


def scale_of(h):
    return lax.rsqrt(jnp.mean(h * h, 0, keepdims=True) + 1e-6)


def normed(h):
    wide = h.astype(f32)
    return (wide * scale_of(wide)).astype(bf16)


STEPS = 8


def adamw_kernel(*refs):
    w, m, v, g, new_w, new_m, new_v = (refs[i : i + 7] for i in range(0, 49, 7))
    for n in range(7):

        def some(i, _):
            here = pl.ds(pl.multiple_of(i * 16, 16), 16)
            grad, wide = g[n][here, :].astype(f32), w[n][0, here, :].astype(f32)
            first = 0.9 * m[n][0, here, :] + 0.1 * grad
            second = 0.95 * v[n][0, here, :] + 0.05 * grad * grad
            step = first * lax.rsqrt(second + 1e-8) + 0.1 * wide
            new_w[n][0, here, :] = (wide - 0.02 * step).astype(bf16)
            new_m[n][0, here, :], new_v[n][0, here, :] = first, second

        lax.fori_loop(0, g[n].shape[0] // 16, some, None)


def adamw(w, m, v, g):
    flat = [pl.BlockSpec((x.shape[0] // STEPS, x.shape[1]), lambda i: (i, 0)) for x in g]
    deep = [pl.BlockSpec((1, x.shape[0] // STEPS, x.shape[1]), lambda i: (0, i, 0)) for x in g]
    return pl.pallas_call(
        adamw_kernel,
        grid=(STEPS,),
        in_specs=deep * 3 + flat,
        out_specs=deep * 3,
        out_shape=[jax.ShapeDtypeStruct(x.shape, x.dtype) for x in (*w, *m, *v)],
        compiler_params=pltpu.CompilerParams(vmem_limit_bytes=60 * 2**20),
        name="adamw",
    )(*w, *m, *v, *g)


def hidden():
    return lax.broadcasted_iota(jnp.int32, (QB, QB), 0) > lax.broadcasted_iota(jnp.int32, (QB, QB), 1)


def turn(t, cos, sin):
    a, b = t[:HALF].astype(f32), t[HALF:].astype(f32)
    return jnp.concatenate([a * cos - b * sin, b * cos + a * sin], 0).astype(bf16)


def attend_kernel(q_in, k_in, v_ref, cos_ref, sin_ref, out_ref, lse_ref, q_ref, kt_ref, k_ref, v_out):
    @pl.when(pl.program_id(0) == 0)
    def _():
        kt_ref[...] = turn(k_in[...], cos_ref[...], sin_ref[...])
        k_ref[...] = kt_ref[...].T
        v_out[...] = v_ref[...].T

    q_ref[...] = turn(q_in[...], cos_ref[...], sin_ref[...])
    for i in range(TOKENS // QB):
        cols, seen = slice(i * QB, (i + 1) * QB), i * QB
        q = q_ref[:, cols]
        edge = jnp.where(hidden(), -1e30, dot(k_ref[cols, :], q))
        top = edge.max(0, keepdims=True)
        if seen:
            past = dot(k_ref[:seen, :], q)
            top = jnp.maximum(top, past.max(0, keepdims=True))
        p = jnp.exp2((edge - top) * (SCALE * LOG2E))
        total, got = p.sum(0, keepdims=True), dot(v_ref[:, cols], p.astype(bf16))
        if seen:
            p = jnp.exp2((past - top) * (SCALE * LOG2E))
            total, got = total + p.sum(0, keepdims=True), got + dot(v_ref[:, :seen], p.astype(bf16))
        out_ref[:, cols] = (got * (1 / total)).astype(bf16)
        lse_ref[0, :, cols] = top * SCALE + jnp.log(total)


def attend(qkv, cos, sin):
    table, tall = pl.BlockSpec((HALF, TOKENS), lambda i: (0, 0)), pl.BlockSpec((TOKENS, HEAD), lambda i: (0, 0))
    row = lambda at: pl.BlockSpec((HEAD, TOKENS), at)
    each = row(lambda i: (i, 0))
    like = jax.ShapeDtypeStruct
    return pl.pallas_call(
        attend_kernel,
        grid=(HEADS,),
        in_specs=[each, row(lambda i: (HEADS, 0)), row(lambda i: (HEADS + 1, 0)), table, table],
        out_specs=[each, pl.BlockSpec((1, 1, TOKENS), lambda i: (i, 0, 0)), each, row(lambda i: (0, 0)), tall, tall],
        out_shape=[like((D, TOKENS), bf16), like((HEADS, 1, TOKENS), f32), like((D, TOKENS), bf16), like((HEAD, TOKENS), bf16),
                   like((TOKENS, HEAD), bf16), like((TOKENS, HEAD), bf16)],
        compiler_params=pltpu.CompilerParams(vmem_limit_bytes=32 * 2**20),
        name="attend",
    )(qkv, qkv, qkv, cos, sin)


def norm_all(to, source):
    def some(i, _):
        cols = pl.ds(pl.multiple_of(i * HEAD, HEAD), HEAD)
        to[:, cols] = normed(source[:, cols])

    lax.fori_loop(0, TOKENS // HEAD, some, None)


def hidden_kernel(wg_ref, wu_ref, wd_ref, h_ref, dy_ref, act_ref, dg_ref, du_ref, b_ref):
    @pl.when(pl.program_id(0) == 0)
    def _():
        norm_all(b_ref, h_ref)

    gate, up = dot(wg_ref[...], b_ref[...], 0, 0), dot(wu_ref[...], b_ref[...], 0, 0)
    back = dot_t(wd_ref[...], dy_ref[...]).astype(bf16).astype(f32)
    sig = 1 / (1 + jnp.exp(-gate))
    silu = gate * sig
    act_ref[...] = (silu * up).astype(bf16)
    du_ref[...] = (back * silu).astype(bf16)
    dg_ref[...] = (back * up * (sig + silu * (1 - sig))).astype(bf16)


def hidden_units(wg, wu, wd, h, dy):
    wide, whole = pl.BlockSpec((D, QB), lambda i: (0, i)), lambda x: pl.BlockSpec(x.shape, lambda i: (0, 0))
    out = pl.BlockSpec((QB, TOKENS), lambda i: (i, 0))
    return pl.pallas_call(
        hidden_kernel,
        grid=(FF // QB,),
        in_specs=[wide, wide, pl.BlockSpec((QB, D), lambda i: (i, 0)), whole(h), whole(dy)],
        out_specs=[out] * 3 + [whole(h)],
        out_shape=[jax.ShapeDtypeStruct((FF, TOKENS), bf16)] * 3 + [jax.ShapeDtypeStruct(h.shape, bf16)],
        compiler_params=pltpu.CompilerParams(vmem_limit_bytes=62 * 2**20),
        name="hidden_units",
    )(wg, wu, wd, h, dy)


class Unit:
    def __init__(self, number, wave, colour, row0, rows, cols):
        self.n, self.wave, self.axes, self.row0, self.R, self.W = number, wave, tuple((colour + i) % 3 for i in range(3)), row0, rows, cols
        self.Rb = rows // 4
        self.h = -(-self.Rb // 32) * 16


def waves_of():
    got = [[Unit(c, 0, c, row0, rows, D) for c, (row0, rows) in enumerate(CUTS)]]
    for wave, cols in ((1, PART), (2, PART), (3, 512)):
        got.append([Unit(3 * wave + c, wave, c, row0, rows, cols) for c, (row0, rows) in enumerate(SLABS)])
    return got


def pieces(u):
    r = slice(u.row0, u.row0 + u.R)
    if u.wave == 0:
        return [(6, slice(j * PART + u.row0, j * PART + u.row0 + u.R), slice(0, D), j, slice(0, D)) for j in range(4)]
    if u.wave < 3:
        return [(3 + u.wave, r, slice(j * PART, (j + 1) * PART), j, slice(0, PART)) for j in range(4)]
    cut = ((0, 0, 512, 0, 0), (0, 512, D, 1, 0), (1, 0, HEAD, 1, 384), (2, 0, HEAD, 2, 0), (3, 0, 384, 2, HEAD), (3, 384, D, 3, 0))
    return [(a, r, slice(c0, c1), j, slice(b0, b0 + c1 - c0)) for a, c0, c1, j, b0 in cut]


class Comm:
    def __init__(self, units, bufs, ssem, rsem):
        self.units, self.bufs, self.ssem, self.rsem = units, bufs, ssem, rsem
        self.rep, self.me = lax.axis_index("rep"), lax.axis_index("dp")
        self.at = [lax.rem(lax.div(self.me, s), 4) for s in STRIDES]

    def place(self, u, stage):
        p = self.at[u.axes[stage]]
        return p, lax.rem(p + 1, 4), lax.rem(p + 3, 4), lax.rem(p + 2, 4)

    def neighbour(self, axis, by):
        p = self.at[axis]
        return self.me + (lax.rem(p + by, 4) - p) * STRIDES[axis]

    def greet(self):
        sem = pltpu.get_barrier_semaphore()
        for axis in range(3):
            for by in (1, 3):
                pl.semaphore_signal(sem, inc=1, device_id=(self.rep, self.neighbour(axis, by)), device_id_type=MESH_ID)

    def met(self):
        pl.semaphore_wait(pltpu.get_barrier_semaphore(), 6)

    def copy(self, u, stage, k, src, dst, by):
        return pltpu.make_async_remote_copy(src_ref=src, dst_ref=dst, send_sem=self.ssem.at[u.n, k], recv_sem=self.rsem.at[u.n, k],
                                            device_id=(self.rep, self.neighbour(u.axes[stage], by)), device_id_type=MESH_ID)

    def send(self, u, stage, k, src, dst, by):
        self.copy(u, stage, k, src, dst, by).start()

    def got(self, u, stage, k, dst):
        self.copy(u, stage, k, dst, dst, 1).wait_recv()

    def done_sending(self, u, stage, k, parts):
        for i, part in enumerate(parts):
            self.copy(u, stage, k + i, part, part, 1).wait_send()

    @staticmethod
    def rows(ref, start, n):
        return ref.at[pl.ds(start if isinstance(start, int) else pl.multiple_of(start, 16), n), :]

    @staticmethod
    def each(n, f):
        rows = next(size for size in (64, 48, 32, 16) if n % size == 0)

        def body(i, _):
            f(pl.multiple_of(i * rows, 16), rows)

        lax.fori_loop(0, n // rows, body, None)

    def scatter_start(self, u, stage):
        b = self.bufs[u.n]
        p, r, l, o = self.place(u, stage)
        if stage == 0:
            size, h, src = u.R, u.R // 2, lambda j, at, n: self.rows(b.own.at[j], at, n)
            ro, rr = b.r1o, b.r1
        else:
            size, h, src = u.Rb, u.h, lambda j, at, n: self.rows(b.r1o, j * u.Rb + at, n)
            ro, rr = b.r2o, b.r2
        k = 6 * stage
        self.send(u, stage, k, src(o, 0, h), ro.at[0:h], 1)
        self.send(u, stage, k + 1, src(o, h, size - h), ro.at[h:size], 3)
        self.send(u, stage, k + 2, src(r, h, size - h), rr.at[0, h:size], 1)
        self.send(u, stage, k + 3, src(l, 0, h), rr.at[1, 0:h], 3)

    def scatter_combine(self, u, stage):
        b = self.bufs[u.n]
        p, r, l, o = self.place(u, stage)
        size, h, ro, rr = (u.R, u.R // 2, b.r1o, b.r1) if stage == 0 else (u.Rb, u.h, b.r2o, b.r2)
        k = 6 * stage
        for step, (j, lo, n, by, slot) in enumerate(((r, 0, h, 1, 0), (l, h, size - h, 3, 1))):
            self.got(u, stage, k + step, ro.at[lo : lo + n])

            def add(i, size):
                here = pl.ds(pl.multiple_of(lo + i, 16), size)
                ro[here, :] = (self.term(u, stage, j, lo + i, size) + ro[here, :].astype(jnp.float32)).astype(jnp.bfloat16)

            self.each(n, add)
            self.send(u, stage, k + 4 + step, ro.at[lo : lo + n], rr.at[slot, lo : lo + n], by)

    def term(self, u, stage, j, at, size):
        b = self.bufs[u.n]
        if stage == 0:
            return b.own[j, pl.ds(pl.multiple_of(at, 16), size), :].astype(jnp.float32)
        here = pl.ds(pl.multiple_of(j * u.Rb + at, 16), size)
        return self.first_sum(u, here)

    def first_sum(self, u, here):
        b = self.bufs[u.n]
        mine = self.place(u, 0)[0]
        return b.own[mine, here, :].astype(jnp.float32) + b.r1[0, here, :].astype(jnp.float32) + b.r1[1, here, :].astype(jnp.float32)

    def scatter_wait(self, u, stage):
        b = self.bufs[u.n]
        size, h, rr = (u.R, u.R // 2, b.r1) if stage == 0 else (u.Rb, u.h, b.r2)
        k = 6 * stage
        self.got(u, stage, k + 2, rr.at[0, h:size])
        self.got(u, stage, k + 3, rr.at[1, 0:h])
        self.got(u, stage, k + 4, rr.at[0, 0:h])
        self.got(u, stage, k + 5, rr.at[1, h:size])
        one, other = (b.r1o, b.r2o)[stage].at[0:h], (b.r1o, b.r2o)[stage].at[h:size]
        self.done_sending(u, stage, k, (one, other, other, one, one, other))

    def first_end(self, u):
        b = self.bufs[u.n]
        self.scatter_wait(u, 0)

        def add(i, size):
            here = pl.ds(i, size)
            b.r1o[here, :] = self.first_sum(u, here).astype(jnp.bfloat16)

        self.each(u.R, add)
        self.scatter_start(u, 1)

    def second_end(self, u):
        b = self.bufs[u.n]
        self.scatter_wait(u, 1)
        mine, slot = self.place(u, 1)[0], self.place(u, 2)[0]

        def add(i, size):
            here = pl.ds(i, size)
            total = self.term(u, 1, mine, i, size) + b.r2[0, here, :].astype(jnp.float32) + b.r2[1, here, :].astype(jnp.float32)
            b.t3[slot, here, :] = total.astype(jnp.bfloat16)

        self.each(u.Rb, add)
        self.gather_start(u, 2)

    def region(self, u, stage):
        b = self.bufs[u.n]
        if stage == 2:
            return (lambda j, at, n: b.t3.at[j, at : at + n]), u.Rb, u.h, 12
        if stage == 1:
            mine = self.place(u, 0)[0]
            return (lambda j, at, n: self.rows(b.own.at[mine], j * u.Rb + at, n)), u.Rb, u.h, 16
        return (lambda j, at, n: b.own.at[j, at : at + n]), u.R, u.R // 2, 20

    def gather_start(self, u, stage):
        part, size, h, k = self.region(u, stage)
        p, r, l, o = self.place(u, stage)
        self.send(u, stage, k, part(p, 0, size), part(p, 0, size), 1)
        self.send(u, stage, k + 1, part(p, 0, size), part(p, 0, size), 3)

    def gather_forward(self, u, stage):
        part, size, h, k = self.region(u, stage)
        p, r, l, o = self.place(u, stage)
        self.got(u, stage, k, part(l, 0, size))
        self.send(u, stage, k + 2, part(l, 0, h), part(l, 0, h), 1)
        self.got(u, stage, k + 1, part(r, 0, size))
        self.send(u, stage, k + 3, part(r, h, size - h), part(r, h, size - h), 3)

    def gather_wait(self, u, stage):
        part, size, h, k = self.region(u, stage)
        p, r, l, o = self.place(u, stage)
        self.got(u, stage, k + 2, part(o, 0, h))
        self.got(u, stage, k + 3, part(o, h, size - h))
        self.done_sending(u, stage, k, (part(p, 0, size), part(p, 0, size), part(l, 0, h), part(r, h, size - h)))

    def third_end(self, u):
        b = self.bufs[u.n]
        self.gather_wait(u, 2)
        first, second = self.place(u, 0)[0], self.place(u, 1)[0]

        def add(i, size):
            here = pl.ds(i, size)
            a, c, d, e = (b.t3[j, here, :].astype(jnp.float32) for j in range(4))
            b.own[first, pl.ds(pl.multiple_of(second * u.Rb + i, 16), size), :] = (a + c + d + e).astype(jnp.bfloat16)

        self.each(u.Rb, add)
        self.gather_start(u, 1)

    def fourth_end(self, u):
        self.gather_wait(u, 1)
        self.gather_start(u, 0)

    def stage(self, wave, number):
        steps = ((self.scatter_start, 0), (self.scatter_combine, 0), (self.first_end,), (self.scatter_combine, 1), (self.second_end,),
                 (self.gather_forward, 2), (self.third_end,), (self.gather_forward, 1), (self.fourth_end,), (self.gather_forward, 0), (self.gather_wait, 0))
        for u in wave:
            steps[number][0](u, *steps[number][1:])


class Bufs:
    def __init__(self, refs):
        self.own, self.r1o, self.r1, self.r2o, self.r2, self.t3 = refs


def unit_scratch(u):
    shapes = ((4, u.R, u.W), (u.R, u.W), (2, u.R, u.W), (u.Rb, u.W), (2, u.Rb, u.W), (4, u.Rb, u.W))
    return [pltpu.VMEM(s, bf16) for s in shapes]


BESIDE = "//1//1/0///12//10/2/10/2/1/120/1/0".split("/")
AFTER = "32032302313230312320303"


class Pacer:
    def __init__(self, comm, waves, finish):
        self.comm, self.waves, self.finish = comm, waves, finish
        self.next, self.plan = {}, list(BESIDE)

    def launch(self, w):
        self.comm.stage(self.waves[w], 0)
        self.next[w] = 1

    def advance(self, order):
        for w in map(int, order):
            self.comm.stage(self.waves[w], self.next[w])
            self.next[w] += 1
            if self.next[w] == LAST:
                self.finish(w)

    def tick(self):
        self.advance(self.plan.pop(0))


def turn_back(d, cos, sin):
    d = d.astype(bf16).astype(f32)
    a, b = d[:HALF], d[HALF:]
    return jnp.concatenate([a * cos + b * sin, b * cos - a * sin], 0).astype(bf16)


def main_kernel(act, dg, du, dy, b, h, out, x, q, kt, k, v, lse, cos, sin, wg, wu, wo, *refs):
    waves = waves_of()
    units = [u for wave in waves for u in wave]
    outs, scratch = refs[:7], refs[7:]
    bufs = [Bufs(scratch[6 * n : 6 * n + 6]) for n in range(len(units))]
    ssem, rsem, osem, dy_s, db_s, csem, wsem, isem = scratch[6 * len(units) :]
    comm = Comm(units, bufs, ssem, rsem)
    comm.greet()

    def results(u):
        for i, (n, r, c, j, cols) in enumerate(pieces(u)):
            yield pltpu.make_async_copy(bufs[u.n].own.at[j, :, cols], outs[n].at[r, c], osem.at[u.n, i])

    def finish(w):
        for u in waves[w]:
            for copy in results(u):
                copy.start()

    pacer = Pacer(comm, waves, finish)

    def keep(w, j, cols, got):
        for u in waves[w]:
            bufs[u.n].own[j, :, cols] = got[u.row0 : u.row0 + u.R].astype(bf16)

    def first(chunk, weight, b_s):
        dy_in, b_in = pltpu.make_async_copy(dy, dy_s, isem.at[0]), pltpu.make_async_copy(b, b_s, isem.at[1])
        groups = [(0, 0, False)] + [(w, j, back) for back in (False, True) for w in (1, 2) for j in (0, 2)]

        def loads(g):
            w, start, back = groups[g]
            for i in range(4 if w == 0 else 2):
                slot, j = (i, i) if w == 0 else (g % 2 * 2 + i, start + i)
                yield pltpu.make_async_copy((act, dg, du)[w].at[j * PART : (j + 1) * PART, :], chunk.at[slot], csem.at[slot])
                if back:
                    yield pltpu.make_async_copy((wg, wu)[w - 1].at[:, j * PART : (j + 1) * PART], weight.at[slot], wsem.at[slot])

        def run(g):
            w, start, back = groups[g]

            def body(i, _):
                slot, j = g % 2 * 2 + i, start + i
                if w == 0:
                    keep(0, i, slice(0, D), dot(chunk[i], dy_s[...]))
                elif not back:
                    keep(w, j, slice(0, PART), dot_t(b_s[...], chunk[slot]))
                else:

                    def some(n, _):
                        cols = pl.ds(pl.multiple_of(n * QB, QB), QB)
                        db_s[:, cols] += dot(weight[slot], chunk[slot, :, cols])

                    lax.fori_loop(0, TOKENS // QB, some, None)

            if back:
                for i in range(2):
                    body(i, None)
                    pacer.tick()
            else:
                lax.fori_loop(0, 4 if w == 0 else 2, body, None)

        for copy in [dy_in, *loads(0), b_in]:
            copy.start()
        db_s[...] = jnp.zeros_like(db_s)
        dy_in.wait()
        for g, (w, start, back) in enumerate(groups):
            ahead = loads(g + 1) if 0 < g < len(groups) - 1 else ()
            for copy in ahead:
                copy.start()
            for copy in loads(g):
                copy.wait()
            if (w, start, back) == (1, 0, False):
                b_in.wait()
            run(g)
            if w == 0:
                for copy in loads(1):
                    copy.start()
                comm.met()
            if not back and start == (2 if w else 0):
                pacer.launch(w)
            if w and not back:
                pacer.tick()

    def second(h_s, out_s, wo_s, q_s, kt_s, k_s, v_s, lse_s, cos_s, sin_s, dout_s, dqkv_s, dk_s, dv_s, delta_s):
        near, far = (h_s, out_s, wo_s, q_s, kt_s, k_s, v_s, lse_s, cos_s, sin_s), (h, out, wo, q, kt, k, v, lse, cos, sin)
        ins = [pltpu.make_async_copy(x, y, isem.at[n]) for n, (x, y) in enumerate(zip(far, near))]
        for copy in ins:
            copy.start()
        dk_s[...] = jnp.zeros_like(dk_s)
        dv_s[...] = jnp.zeros_like(dv_s)
        for copy in ins:
            copy.wait()

        def through_norm(i, _):
            cols = pl.ds(pl.multiple_of(i * HEAD, HEAD), HEAD)
            x, g = h_s[:, cols].astype(f32), db_s[:, cols].astype(bf16).astype(f32)
            s = scale_of(x)
            d = g * s - x * (s * s * s * jnp.mean(g * x, 0, keepdims=True))
            h_s[:, cols] = (d.astype(bf16).astype(f32) + dy_s[cols, :].T.astype(f32)).astype(bf16)

        lax.fori_loop(0, TOKENS // HEAD, through_norm, None)
        pacer.tick()
        dout_s[...] = dot(wo_s[...], h_s[...]).astype(bf16)
        pacer.tick()
        keep(3, 2, slice(HEAD, 512), dot_t(out_s[...], h_s[:384, :]))
        keep(3, 3, slice(0, 512), dot_t(out_s[...], h_s[384:, :]))
        pacer.tick()
        for n in range(HEADS):
            rows = slice(n * HEAD, (n + 1) * HEAD)
            delta_s[n] = (dout_s[rows, :].astype(f32) * out_s[rows, :].astype(f32)).sum(0, keepdims=True)
        x_in = pltpu.make_async_copy(x, out_s, isem.at[1])
        x_in.start()

        def head(n, _):
            rows = pl.ds(pl.multiple_of(n * HEAD, HEAD), HEAD)
            for i in range(TOKENS // QB):
                cols, seen = slice(i * QB, (i + 1) * QB), i * QB
                qi, do = q_s[rows, cols], dout_s[rows, cols]
                top, delta = lse_s[n][:, cols] * LOG2E, delta_s[n][:, cols]
                dq = None
                for keys in [slice(0, seen), cols] if seen else [cols]:
                    p = jnp.exp2(dot(k_s[keys, :], qi) * (SCALE * LOG2E) - top)
                    if keys is cols:
                        p = jnp.where(hidden(), 0.0, p)
                    ds = (p * (dot(v_s[keys, :], do) - delta)).astype(bf16)
                    dv_s[:, keys] += dot_t(do, p.astype(bf16))
                    dk_s[:, keys] += dot_t(qi, ds)
                    part = dot(kt_s[:, keys], ds)
                    dq = part if dq is None else dq + part
                dqkv_s[rows, cols] = turn_back(dq * SCALE, cos_s[:, cols], sin_s[:, cols])

        for first_head, end in ((0, 2), (2, 4), (4, HEADS)):
            lax.fori_loop(first_head, end, head, None)
            pacer.tick()
        dqkv_s[D : D + HEAD, :] = turn_back(dk_s[...] * SCALE, cos_s[...], sin_s[...])
        dqkv_s[D + HEAD :, :] = dv_s[...].astype(bf16)
        x_in.wait()
        norm_all(out_s, out_s)

        def block(j, _):
            keep(3, j, slice(0, 512), dot_t(out_s[...], dqkv_s[pl.ds(pl.multiple_of(j * 512, 512), 512), :]))

        lax.fori_loop(0, 2, block, None)
        keep(3, 2, slice(0, HEAD), dot_t(out_s[...], dqkv_s[D + HEAD :, :]))
        pacer.launch(3)

    wide = pltpu.VMEM((D, TOKENS), bf16)
    pl.run_scoped(first, pltpu.VMEM((4, PART, TOKENS), bf16), pltpu.VMEM((4, D, PART), bf16), wide)
    small, tall = pltpu.VMEM((HEAD, TOKENS), bf16), pltpu.VMEM((TOKENS, HEAD), bf16)
    table, row = pltpu.VMEM((HALF, TOKENS), f32), pltpu.VMEM((HEADS, 1, TOKENS), f32)
    sums = pltpu.VMEM((HEAD, TOKENS), f32)
    pl.run_scoped(second, wide, wide, pltpu.VMEM((D, D), bf16), wide, small, tall, tall, row, table, table, wide, pltpu.VMEM((QKV, TOKENS), bf16), sums, sums, row)
    pacer.advance(AFTER)
    for u in units:
        for copy in results(u):
            copy.wait()


def gradients(*arrays):
    units = [u for wave in waves_of() for u in wave]
    anywhere = pl.BlockSpec(memory_space=pl.ANY)
    shapes = ((D, D), (D, HEAD), (D, HEAD), (D, D), (D, FF), (D, FF), (FF, D))
    dma = pltpu.SemaphoreType.DMA
    return pl.pallas_call(
        main_kernel,
        out_shape=[jax.ShapeDtypeStruct(s, bf16) for s in shapes],
        in_specs=[anywhere] * len(arrays),
        out_specs=[anywhere] * len(shapes),
        scratch_shapes=[s for u in units for s in unit_scratch(u)]
        + [dma((len(units), 24)), dma((len(units), 24)), dma((len(units), 6)), pltpu.VMEM((TOKENS, D), bf16), pltpu.VMEM((D, TOKENS), f32), dma((4,)), dma((4,)), dma((10,))],
        compiler_params=pltpu.CompilerParams(collective_id=0, has_side_effects=True, vmem_limit_bytes=63 * 2**20),
        name="gradients",
    )(*arrays)


def solution(mesh):
    def step(x, dy, *arrays):
        weights, m, v = (arrays[i : i + 7] for i in (0, 7, 14))
        wq, wk, wv, wo, wg, wu, wd = (w[0] for w in weights)
        x, dy = x[0].T, dy[0]
        angle = jnp.arange(TOKENS, dtype=f32)[None, :] * THETA ** (-jnp.arange(HALF, dtype=f32) / HALF)[:, None]
        cos, sin = jnp.cos(angle), jnp.sin(angle)
        a = normed(x)
        qkv = dot(jnp.concatenate([wq, wk, wv], 1), a, 0, 0).astype(bf16)
        out, lse, q, kt, k, v_tall = attend(qkv, cos, sin)
        h = x + dot(wo, out, 0, 0).astype(bf16)
        act, dg, du, b = hidden_units(wg, wu, wd, h, dy)
        summed = gradients(act, dg, du, dy, b, h, out, x, q, kt, k, v_tall, lse, cos, sin, wg, wu, wo)
        return tuple(adamw(weights, m, v, summed))

    states, all_of = P(("rep", "dp"), None, None), P(None, None, None)
    return jax.shard_map(
        step,
        mesh=mesh,
        in_specs=(states, states) + (all_of,) * 21,
        out_specs=(P("rep", None, None),) * 21,
        check_vma=False,
    )
```

```python
import functools

import jax
import jax.numpy as jnp
import numpy as np
from jax import lax
from jax.experimental import pallas as pl
from jax.experimental.pallas import tpu as pltpu
from jax.sharding import PartitionSpec as P

HEAD = 128
HALF = HEAD // 2
HEADS = 7
THETA = 10000
TOKENS = 1024
D, FF, QKV = 896, 2560, 1152
QB = 256
PART = FF // 4
SCALE = HEAD**-0.5
LOG2E = 1.4426950408889634
LAST = 11
STRIDES = (16, 4, 1)
MESH_ID = pl.DeviceIdType.MESH
SLABS = ((0, 256), (256, 320), (576, 320))
CUTS = ((0, 256), (256, 192), (448, 192))
bf16, f32 = jnp.bfloat16, jnp.float32


def dot(a, b, ca=1, cb=0):
    return lax.dot_general(a, b, (((ca,), (cb,)), ((), ())), preferred_element_type=f32)


def dot_t(a, b):
    return dot(a, b, 1, 1)


def scale_of(h):
    return lax.rsqrt(jnp.mean(h * h, 0, keepdims=True) + 1e-6)


def normed(h):
    wide = h.astype(f32)
    return (wide * scale_of(wide)).astype(bf16)


STEPS = 8


def adamw_kernel(*refs):
    w, m, v, g, new_w, new_m, new_v = (refs[i : i + 7] for i in range(0, 49, 7))
    for n in range(7):

        def some(i, _):
            here = pl.ds(pl.multiple_of(i * 16, 16), 16)
            grad, wide = g[n][here, :].astype(f32), w[n][0, here, :].astype(f32)
            first = 0.9 * m[n][0, here, :] + 0.1 * grad
            second = 0.95 * v[n][0, here, :] + 0.05 * grad * grad
            step = first * lax.rsqrt(second + 1e-8) + 0.1 * wide
            new_w[n][0, here, :] = (wide - 0.02 * step).astype(bf16)
            new_m[n][0, here, :], new_v[n][0, here, :] = first, second

        lax.fori_loop(0, g[n].shape[0] // 16, some, None)


def adamw(w, m, v, g):
    flat = [pl.BlockSpec((x.shape[0] // STEPS, x.shape[1]), lambda i: (i, 0)) for x in g]
    deep = [pl.BlockSpec((1, x.shape[0] // STEPS, x.shape[1]), lambda i: (0, i, 0)) for x in g]
    return pl.pallas_call(
        adamw_kernel,
        grid=(STEPS,),
        in_specs=deep * 3 + flat,
        out_specs=deep * 3,
        out_shape=[jax.ShapeDtypeStruct(x.shape, x.dtype) for x in (*w, *m, *v)],
        compiler_params=pltpu.CompilerParams(vmem_limit_bytes=60 * 2**20),
        name="adamw",
    )(*w, *m, *v, *g)


def hidden():
    return lax.broadcasted_iota(jnp.int32, (QB, QB), 0) > lax.broadcasted_iota(jnp.int32, (QB, QB), 1)


def turn(t, cos, sin):
    a, b = t[:HALF].astype(f32), t[HALF:].astype(f32)
    return jnp.concatenate([a * cos - b * sin, b * cos + a * sin], 0).astype(bf16)


def attend_kernel(q_in, k_in, v_ref, cos_ref, sin_ref, out_ref, lse_ref, q_ref, kt_ref, k_ref, v_out):
    @pl.when(pl.program_id(0) == 0)
    def _():
        kt_ref[...] = turn(k_in[...], cos_ref[...], sin_ref[...])
        k_ref[...] = kt_ref[...].T
        v_out[...] = v_ref[...].T

    q_ref[...] = turn(q_in[...], cos_ref[...], sin_ref[...])
    for i in range(TOKENS // QB):
        cols, seen = slice(i * QB, (i + 1) * QB), i * QB
        q = q_ref[:, cols]
        edge = jnp.where(hidden(), -1e30, dot(k_ref[cols, :], q))
        top = edge.max(0, keepdims=True)
        if seen:
            past = dot(k_ref[:seen, :], q)
            top = jnp.maximum(top, past.max(0, keepdims=True))
        p = jnp.exp2((edge - top) * (SCALE * LOG2E))
        total, got = p.sum(0, keepdims=True), dot(v_ref[:, cols], p.astype(bf16))
        if seen:
            p = jnp.exp2((past - top) * (SCALE * LOG2E))
            total, got = total + p.sum(0, keepdims=True), got + dot(v_ref[:, :seen], p.astype(bf16))
        out_ref[:, cols] = (got * (1 / total)).astype(bf16)
        lse_ref[0, :, cols] = top * SCALE + jnp.log(total)


def attend(qkv, cos, sin):
    table, tall = pl.BlockSpec((HALF, TOKENS), lambda i: (0, 0)), pl.BlockSpec((TOKENS, HEAD), lambda i: (0, 0))
    row = lambda at: pl.BlockSpec((HEAD, TOKENS), at)
    each = row(lambda i: (i, 0))
    like = jax.ShapeDtypeStruct
    return pl.pallas_call(
        attend_kernel,
        grid=(HEADS,),
        in_specs=[each, row(lambda i: (HEADS, 0)), row(lambda i: (HEADS + 1, 0)), table, table],
        out_specs=[each, pl.BlockSpec((1, 1, TOKENS), lambda i: (i, 0, 0)), each, row(lambda i: (0, 0)), tall, tall],
        out_shape=[like((D, TOKENS), bf16), like((HEADS, 1, TOKENS), f32), like((D, TOKENS), bf16), like((HEAD, TOKENS), bf16),
                   like((TOKENS, HEAD), bf16), like((TOKENS, HEAD), bf16)],
        compiler_params=pltpu.CompilerParams(vmem_limit_bytes=32 * 2**20),
        name="attend",
    )(qkv, qkv, qkv, cos, sin)


def norm_all(to, source):
    def some(i, _):
        cols = pl.ds(pl.multiple_of(i * HEAD, HEAD), HEAD)
        to[:, cols] = normed(source[:, cols])

    lax.fori_loop(0, TOKENS // HEAD, some, None)


def hidden_kernel(wg_ref, wu_ref, wd_ref, b_ref, dy_ref, act_ref, dg_ref, du_ref):
    gate, up = dot(wg_ref[...], b_ref[...], 0, 0), dot(wu_ref[...], b_ref[...], 0, 0)
    back = dot_t(wd_ref[...], dy_ref[...]).astype(bf16).astype(f32)
    sig = 1 / (1 + jnp.exp(-gate))
    silu = gate * sig
    act_ref[...] = (silu * up).astype(bf16)
    du_ref[...] = (back * silu).astype(bf16)
    dg_ref[...] = (back * up * (sig + silu * (1 - sig))).astype(bf16)


def hidden_units(wg, wu, wd, b, dy):
    wide, whole = pl.BlockSpec((D, QB), lambda i: (0, i)), lambda x: pl.BlockSpec(x.shape, lambda i: (0, 0))
    out = pl.BlockSpec((QB, TOKENS), lambda i: (i, 0))
    return pl.pallas_call(
        hidden_kernel,
        grid=(FF // QB,),
        in_specs=[wide, wide, pl.BlockSpec((QB, D), lambda i: (i, 0)), whole(b), whole(dy)],
        out_specs=[out] * 3,
        out_shape=[jax.ShapeDtypeStruct((FF, TOKENS), bf16)] * 3,
        compiler_params=pltpu.CompilerParams(vmem_limit_bytes=62 * 2**20),
        name="hidden_units",
    )(wg, wu, wd, b, dy)


class Unit:
    def __init__(self, number, wave, colour, row0, rows, cols):
        self.n, self.wave, self.axes, self.row0, self.R, self.W = number, wave, tuple((colour + i) % 3 for i in range(3)), row0, rows, cols
        self.Rb = rows // 4
        self.h = -(-self.Rb // 32) * 16


def waves_of():
    got = [[Unit(c, 0, c, row0, rows, D) for c, (row0, rows) in enumerate(CUTS)]]
    for wave, cols in ((1, PART), (2, PART), (3, 512)):
        got.append([Unit(3 * wave + c, wave, c, row0, rows, cols) for c, (row0, rows) in enumerate(SLABS)])
    return got


def pieces(u):
    r = slice(u.row0, u.row0 + u.R)
    if u.wave == 0:
        return [(6, slice(j * PART + u.row0, j * PART + u.row0 + u.R), slice(0, D), j, slice(0, D)) for j in range(4)]
    if u.wave < 3:
        return [(3 + u.wave, r, slice(j * PART, (j + 1) * PART), j, slice(0, PART)) for j in range(4)]
    cut = ((0, 0, 512, 0, 0), (0, 512, D, 1, 0), (1, 0, HEAD, 1, 384), (2, 0, HEAD, 2, 0), (3, 0, 384, 2, HEAD), (3, 384, D, 3, 0))
    return [(a, r, slice(c0, c1), j, slice(b0, b0 + c1 - c0)) for a, c0, c1, j, b0 in cut]


class Comm:
    def __init__(self, units, bufs, ssem, rsem):
        self.units, self.bufs, self.ssem, self.rsem = units, bufs, ssem, rsem
        self.rep, self.me = lax.axis_index("rep"), lax.axis_index("dp")
        self.at = [lax.rem(lax.div(self.me, s), 4) for s in STRIDES]

    def place(self, u, stage):
        p = self.at[u.axes[stage]]
        return p, lax.rem(p + 1, 4), lax.rem(p + 3, 4), lax.rem(p + 2, 4)

    def neighbour(self, axis, by):
        p = self.at[axis]
        return self.me + (lax.rem(p + by, 4) - p) * STRIDES[axis]

    def greet(self):
        sem = pltpu.get_barrier_semaphore()
        for axis in range(3):
            for by in (1, 3):
                pl.semaphore_signal(sem, inc=1, device_id=(self.rep, self.neighbour(axis, by)), device_id_type=MESH_ID)

    def met(self):
        pl.semaphore_wait(pltpu.get_barrier_semaphore(), 6)

    def copy(self, u, stage, k, src, dst, by):
        return pltpu.make_async_remote_copy(src_ref=src, dst_ref=dst, send_sem=self.ssem.at[u.n, k], recv_sem=self.rsem.at[u.n, k],
                                            device_id=(self.rep, self.neighbour(u.axes[stage], by)), device_id_type=MESH_ID)

    def send(self, u, stage, k, src, dst, by):
        self.copy(u, stage, k, src, dst, by).start()

    def got(self, u, stage, k, dst):
        self.copy(u, stage, k, dst, dst, 1).wait_recv()

    def done_sending(self, u, stage, k, parts):
        for i, part in enumerate(parts):
            self.copy(u, stage, k + i, part, part, 1).wait_send()

    @staticmethod
    def rows(ref, start, n):
        return ref.at[pl.ds(start if isinstance(start, int) else pl.multiple_of(start, 16), n), :]

    @staticmethod
    def each(n, f):
        rows = next(size for size in (64, 48, 32, 16) if n % size == 0)

        def body(i, _):
            f(pl.multiple_of(i * rows, 16), rows)

        lax.fori_loop(0, n // rows, body, None)

    def scatter_start(self, u, stage):
        b = self.bufs[u.n]
        p, r, l, o = self.place(u, stage)
        if stage == 0:
            size, h, src = u.R, u.R // 2, lambda j, at, n: self.rows(b.own.at[j], at, n)
            ro, rr = b.r1o, b.r1
        else:
            size, h, src = u.Rb, u.h, lambda j, at, n: self.rows(b.r1o, j * u.Rb + at, n)
            ro, rr = b.r2o, b.r2
        k = 6 * stage
        self.send(u, stage, k, src(o, 0, h), ro.at[0:h], 1)
        self.send(u, stage, k + 1, src(o, h, size - h), ro.at[h:size], 3)
        self.send(u, stage, k + 2, src(r, h, size - h), rr.at[0, h:size], 1)
        self.send(u, stage, k + 3, src(l, 0, h), rr.at[1, 0:h], 3)

    def scatter_combine(self, u, stage):
        b = self.bufs[u.n]
        p, r, l, o = self.place(u, stage)
        size, h, ro, rr = (u.R, u.R // 2, b.r1o, b.r1) if stage == 0 else (u.Rb, u.h, b.r2o, b.r2)
        k = 6 * stage
        for step, (j, lo, n, by, slot) in enumerate(((r, 0, h, 1, 0), (l, h, size - h, 3, 1))):
            self.got(u, stage, k + step, ro.at[lo : lo + n])

            def add(i, size):
                here = pl.ds(pl.multiple_of(lo + i, 16), size)
                ro[here, :] = (self.term(u, stage, j, lo + i, size) + ro[here, :].astype(jnp.float32)).astype(jnp.bfloat16)

            self.each(n, add)
            self.send(u, stage, k + 4 + step, ro.at[lo : lo + n], rr.at[slot, lo : lo + n], by)

    def term(self, u, stage, j, at, size):
        b = self.bufs[u.n]
        if stage == 0:
            return b.own[j, pl.ds(pl.multiple_of(at, 16), size), :].astype(jnp.float32)
        here = pl.ds(pl.multiple_of(j * u.Rb + at, 16), size)
        return self.first_sum(u, here)

    def first_sum(self, u, here):
        b = self.bufs[u.n]
        mine = self.place(u, 0)[0]
        return b.own[mine, here, :].astype(jnp.float32) + b.r1[0, here, :].astype(jnp.float32) + b.r1[1, here, :].astype(jnp.float32)

    def scatter_wait(self, u, stage):
        b = self.bufs[u.n]
        size, h, rr = (u.R, u.R // 2, b.r1) if stage == 0 else (u.Rb, u.h, b.r2)
        k = 6 * stage
        self.got(u, stage, k + 2, rr.at[0, h:size])
        self.got(u, stage, k + 3, rr.at[1, 0:h])
        self.got(u, stage, k + 4, rr.at[0, 0:h])
        self.got(u, stage, k + 5, rr.at[1, h:size])
        one, other = (b.r1o, b.r2o)[stage].at[0:h], (b.r1o, b.r2o)[stage].at[h:size]
        self.done_sending(u, stage, k, (one, other, other, one, one, other))

    def first_end(self, u):
        b = self.bufs[u.n]
        self.scatter_wait(u, 0)

        def add(i, size):
            here = pl.ds(i, size)
            b.r1o[here, :] = self.first_sum(u, here).astype(jnp.bfloat16)

        self.each(u.R, add)
        self.scatter_start(u, 1)

    def second_end(self, u):
        b = self.bufs[u.n]
        self.scatter_wait(u, 1)
        mine, slot = self.place(u, 1)[0], self.place(u, 2)[0]

        def add(i, size):
            here = pl.ds(i, size)
            total = self.term(u, 1, mine, i, size) + b.r2[0, here, :].astype(jnp.float32) + b.r2[1, here, :].astype(jnp.float32)
            b.t3[slot, here, :] = total.astype(jnp.bfloat16)

        self.each(u.Rb, add)
        self.gather_start(u, 2)

    def region(self, u, stage):
        b = self.bufs[u.n]
        if stage == 2:
            return (lambda j, at, n: b.t3.at[j, at : at + n]), u.Rb, u.h, 12
        if stage == 1:
            mine = self.place(u, 0)[0]
            return (lambda j, at, n: self.rows(b.own.at[mine], j * u.Rb + at, n)), u.Rb, u.h, 16
        return (lambda j, at, n: b.own.at[j, at : at + n]), u.R, u.R // 2, 20

    def gather_start(self, u, stage):
        part, size, h, k = self.region(u, stage)
        p, r, l, o = self.place(u, stage)
        self.send(u, stage, k, part(p, 0, size), part(p, 0, size), 1)
        self.send(u, stage, k + 1, part(p, 0, size), part(p, 0, size), 3)

    def gather_forward(self, u, stage):
        part, size, h, k = self.region(u, stage)
        p, r, l, o = self.place(u, stage)
        self.got(u, stage, k, part(l, 0, size))
        self.send(u, stage, k + 2, part(l, 0, h), part(l, 0, h), 1)
        self.got(u, stage, k + 1, part(r, 0, size))
        self.send(u, stage, k + 3, part(r, h, size - h), part(r, h, size - h), 3)

    def gather_wait(self, u, stage):
        part, size, h, k = self.region(u, stage)
        p, r, l, o = self.place(u, stage)
        self.got(u, stage, k + 2, part(o, 0, h))
        self.got(u, stage, k + 3, part(o, h, size - h))
        self.done_sending(u, stage, k, (part(p, 0, size), part(p, 0, size), part(l, 0, h), part(r, h, size - h)))

    def third_end(self, u):
        b = self.bufs[u.n]
        self.gather_wait(u, 2)
        first, second = self.place(u, 0)[0], self.place(u, 1)[0]

        def add(i, size):
            here = pl.ds(i, size)
            a, c, d, e = (b.t3[j, here, :].astype(jnp.float32) for j in range(4))
            b.own[first, pl.ds(pl.multiple_of(second * u.Rb + i, 16), size), :] = (a + c + d + e).astype(jnp.bfloat16)

        self.each(u.Rb, add)
        self.gather_start(u, 1)

    def fourth_end(self, u):
        self.gather_wait(u, 1)
        self.gather_start(u, 0)

    def stage(self, wave, number):
        steps = ((self.scatter_start, 0), (self.scatter_combine, 0), (self.first_end,), (self.scatter_combine, 1), (self.second_end,),
                 (self.gather_forward, 2), (self.third_end,), (self.gather_forward, 1), (self.fourth_end,), (self.gather_forward, 0), (self.gather_wait, 0))
        for u in wave:
            steps[number][0](u, *steps[number][1:])


class Bufs:
    def __init__(self, refs):
        self.own, self.r1o, self.r1, self.r2o, self.r2, self.t3 = refs


def unit_scratch(u):
    shapes = ((4, u.R, u.W), (u.R, u.W), (2, u.R, u.W), (u.Rb, u.W), (2, u.Rb, u.W), (4, u.Rb, u.W))
    return [pltpu.VMEM(s, bf16) for s in shapes]


BESIDE = "//1//1/0///12//10/2/10/2/1/120/1/0".split("/")
AFTER = "32032302313230312320303"


class Pacer:
    def __init__(self, comm, waves, finish):
        self.comm, self.waves, self.finish = comm, waves, finish
        self.next, self.plan = {}, list(BESIDE)

    def launch(self, w):
        self.comm.stage(self.waves[w], 0)
        self.next[w] = 1

    def advance(self, order):
        for w in map(int, order):
            self.comm.stage(self.waves[w], self.next[w])
            self.next[w] += 1
            if self.next[w] == LAST:
                self.finish(w)

    def tick(self):
        self.advance(self.plan.pop(0))


def turn_back(d, cos, sin):
    d = d.astype(bf16).astype(f32)
    a, b = d[:HALF], d[HALF:]
    return jnp.concatenate([a * cos + b * sin, b * cos - a * sin], 0).astype(bf16)


def main_kernel(act, dg, du, dy, b, h, out, x, q, kt, k, v, lse, cos, sin, wg, wu, wo, *refs):
    waves = waves_of()
    units = [u for wave in waves for u in wave]
    outs, scratch = refs[:7], refs[7:]
    bufs = [Bufs(scratch[6 * n : 6 * n + 6]) for n in range(len(units))]
    ssem, rsem, osem, dy_s, db_s, csem, wsem, isem = scratch[6 * len(units) :]
    comm = Comm(units, bufs, ssem, rsem)
    comm.greet()

    def results(u):
        for i, (n, r, c, j, cols) in enumerate(pieces(u)):
            yield pltpu.make_async_copy(bufs[u.n].own.at[j, :, cols], outs[n].at[r, c], osem.at[u.n, i])

    def finish(w):
        for u in waves[w]:
            for copy in results(u):
                copy.start()

    pacer = Pacer(comm, waves, finish)

    def keep(w, j, cols, got):
        for u in waves[w]:
            bufs[u.n].own[j, :, cols] = got[u.row0 : u.row0 + u.R].astype(bf16)

    def first(chunk, weight, b_s):
        dy_in, b_in = pltpu.make_async_copy(dy, dy_s, isem.at[0]), pltpu.make_async_copy(b, b_s, isem.at[1])
        groups = [(0, 0, False)] + [(w, j, back) for back in (False, True) for w in (1, 2) for j in (0, 2)]

        def loads(g):
            w, start, back = groups[g]
            for i in range(4 if w == 0 else 2):
                slot, j = (i, i) if w == 0 else (g % 2 * 2 + i, start + i)
                yield pltpu.make_async_copy((act, dg, du)[w].at[j * PART : (j + 1) * PART, :], chunk.at[slot], csem.at[slot])
                if back:
                    yield pltpu.make_async_copy((wg, wu)[w - 1].at[:, j * PART : (j + 1) * PART], weight.at[slot], wsem.at[slot])

        def run(g):
            w, start, back = groups[g]

            def body(i, _):
                slot, j = g % 2 * 2 + i, start + i
                if w == 0:
                    keep(0, i, slice(0, D), dot(chunk[i], dy_s[...]))
                elif not back:
                    keep(w, j, slice(0, PART), dot_t(b_s[...], chunk[slot]))
                else:

                    def some(n, _):
                        cols = pl.ds(pl.multiple_of(n * QB, QB), QB)
                        db_s[:, cols] += dot(weight[slot], chunk[slot, :, cols])

                    lax.fori_loop(0, TOKENS // QB, some, None)

            if back:
                for i in range(2):
                    body(i, None)
                    pacer.tick()
            else:
                lax.fori_loop(0, 4 if w == 0 else 2, body, None)

        for copy in [dy_in, *loads(0), b_in]:
            copy.start()
        db_s[...] = jnp.zeros_like(db_s)
        dy_in.wait()
        for g, (w, start, back) in enumerate(groups):
            ahead = loads(g + 1) if 0 < g < len(groups) - 1 else ()
            for copy in ahead:
                copy.start()
            for copy in loads(g):
                copy.wait()
            if (w, start, back) == (1, 0, False):
                b_in.wait()
            run(g)
            if w == 0:
                for copy in loads(1):
                    copy.start()
                comm.met()
            if not back and start == (2 if w else 0):
                pacer.launch(w)
            if w and not back:
                pacer.tick()

    def second(h_s, out_s, wo_s, q_s, kt_s, k_s, v_s, lse_s, cos_s, sin_s, dout_s, dqkv_s, dk_s, dv_s, delta_s):
        near, far = (h_s, out_s, wo_s, q_s, kt_s, k_s, v_s, lse_s, cos_s, sin_s), (h, out, wo, q, kt, k, v, lse, cos, sin)
        ins = [pltpu.make_async_copy(x, y, isem.at[n]) for n, (x, y) in enumerate(zip(far, near))]
        for copy in ins:
            copy.start()
        dk_s[...] = jnp.zeros_like(dk_s)
        dv_s[...] = jnp.zeros_like(dv_s)
        for copy in ins:
            copy.wait()

        def through_norm(i, _):
            cols = pl.ds(pl.multiple_of(i * HEAD, HEAD), HEAD)
            x, g = h_s[:, cols].astype(f32), db_s[:, cols].astype(bf16).astype(f32)
            s = scale_of(x)
            d = g * s - x * (s * s * s * jnp.mean(g * x, 0, keepdims=True))
            h_s[:, cols] = (d.astype(bf16).astype(f32) + dy_s[cols, :].T.astype(f32)).astype(bf16)

        lax.fori_loop(0, TOKENS // HEAD, through_norm, None)
        pacer.tick()
        dout_s[...] = dot(wo_s[...], h_s[...]).astype(bf16)
        pacer.tick()
        keep(3, 2, slice(HEAD, 512), dot_t(out_s[...], h_s[:384, :]))
        keep(3, 3, slice(0, 512), dot_t(out_s[...], h_s[384:, :]))
        pacer.tick()
        for n in range(HEADS):
            rows = slice(n * HEAD, (n + 1) * HEAD)
            delta_s[n] = (dout_s[rows, :].astype(f32) * out_s[rows, :].astype(f32)).sum(0, keepdims=True)
        x_in = pltpu.make_async_copy(x, out_s, isem.at[1])
        x_in.start()

        def head(n, _):
            rows = pl.ds(pl.multiple_of(n * HEAD, HEAD), HEAD)
            for i in range(TOKENS // QB):
                cols, seen = slice(i * QB, (i + 1) * QB), i * QB
                qi, do = q_s[rows, cols], dout_s[rows, cols]
                top, delta = lse_s[n][:, cols] * LOG2E, delta_s[n][:, cols]
                dq = None
                for keys in [slice(0, seen), cols] if seen else [cols]:
                    p = jnp.exp2(dot(k_s[keys, :], qi) * (SCALE * LOG2E) - top)
                    if keys is cols:
                        p = jnp.where(hidden(), 0.0, p)
                    ds = (p * (dot(v_s[keys, :], do) - delta)).astype(bf16)
                    dv_s[:, keys] += dot_t(do, p.astype(bf16))
                    dk_s[:, keys] += dot_t(qi, ds)
                    part = dot(kt_s[:, keys], ds)
                    dq = part if dq is None else dq + part
                dqkv_s[rows, cols] = turn_back(dq * SCALE, cos_s[:, cols], sin_s[:, cols])

        for first_head, end in ((0, 2), (2, 4), (4, HEADS)):
            lax.fori_loop(first_head, end, head, None)
            pacer.tick()
        dqkv_s[D : D + HEAD, :] = turn_back(dk_s[...] * SCALE, cos_s[...], sin_s[...])
        dqkv_s[D + HEAD :, :] = dv_s[...].astype(bf16)
        x_in.wait()
        norm_all(out_s, out_s)

        def block(j, _):
            keep(3, j, slice(0, 512), dot_t(out_s[...], dqkv_s[pl.ds(pl.multiple_of(j * 512, 512), 512), :]))

        lax.fori_loop(0, 2, block, None)
        keep(3, 2, slice(0, HEAD), dot_t(out_s[...], dqkv_s[D + HEAD :, :]))
        pacer.launch(3)

    wide = pltpu.VMEM((D, TOKENS), bf16)
    pl.run_scoped(first, pltpu.VMEM((4, PART, TOKENS), bf16), pltpu.VMEM((4, D, PART), bf16), wide)
    small, tall = pltpu.VMEM((HEAD, TOKENS), bf16), pltpu.VMEM((TOKENS, HEAD), bf16)
    table, row = pltpu.VMEM((HALF, TOKENS), f32), pltpu.VMEM((HEADS, 1, TOKENS), f32)
    sums = pltpu.VMEM((HEAD, TOKENS), f32)
    pl.run_scoped(second, wide, wide, pltpu.VMEM((D, D), bf16), wide, small, tall, tall, row, table, table, wide, pltpu.VMEM((QKV, TOKENS), bf16), sums, sums, row)
    pacer.advance(AFTER)
    for u in units:
        for copy in results(u):
            copy.wait()


def gradients(*arrays):
    units = [u for wave in waves_of() for u in wave]
    anywhere = pl.BlockSpec(memory_space=pl.ANY)
    shapes = ((D, D), (D, HEAD), (D, HEAD), (D, D), (D, FF), (D, FF), (FF, D))
    dma = pltpu.SemaphoreType.DMA
    return pl.pallas_call(
        main_kernel,
        out_shape=[jax.ShapeDtypeStruct(s, bf16) for s in shapes],
        in_specs=[anywhere] * len(arrays),
        out_specs=[anywhere] * len(shapes),
        scratch_shapes=[s for u in units for s in unit_scratch(u)]
        + [dma((len(units), 24)), dma((len(units), 24)), dma((len(units), 6)), pltpu.VMEM((TOKENS, D), bf16), pltpu.VMEM((D, TOKENS), f32), dma((4,)), dma((4,)), dma((10,))],
        compiler_params=pltpu.CompilerParams(collective_id=0, has_side_effects=True, vmem_limit_bytes=63 * 2**20),
        name="gradients",
    )(*arrays)


def solution(mesh):
    def step(x, dy, *arrays):
        weights, m, v = (arrays[i : i + 7] for i in (0, 7, 14))
        wq, wk, wv, wo, wg, wu, wd = (w[0] for w in weights)
        x, dy = x[0].T, dy[0]
        angle = jnp.arange(TOKENS, dtype=f32)[None, :] * THETA ** (-jnp.arange(HALF, dtype=f32) / HALF)[:, None]
        cos, sin = jnp.cos(angle), jnp.sin(angle)
        a = normed(x)
        qkv = dot(jnp.concatenate([wq, wk, wv], 1), a, 0, 0).astype(bf16)
        out, lse, q, kt, k, v_tall = attend(qkv, cos, sin)
        h = x + dot(wo, out, 0, 0).astype(bf16)
        b = normed(h)
        act, dg, du = hidden_units(wg, wu, wd, b, dy)
        summed = gradients(act, dg, du, dy, b, h, out, x, q, kt, k, v_tall, lse, cos, sin, wg, wu, wo)
        return tuple(adamw(weights, m, v, summed))

    states, all_of = P(("rep", "dp"), None, None), P(None, None, None)
    return jax.shard_map(
        step,
        mesh=mesh,
        in_specs=(states, states) + (all_of,) * 21,
        out_specs=(P("rep", None, None),) * 21,
        check_vma=False,
    )
```
